128 devices in a mesh: point: 32 (over z_hi, x, y), batch: 4 (over z_lo, core).
Axes of the slice: x: 4, y: 4, z: 4 (z_hi: 2, z_lo: 2; z = z_hi * 2 + z_lo), core: 2. Of those that a mesh axis runs over, the one named last changes fastest.
Arguments:
- activations: bfloat16 [128, 14, 14, 1024], P('batch'), may hold values from -8 to 8
- labels: int32 [128], P('batch'), may hold values from 0 to 999
- t_values: float32 [64], replicated, may hold values from 0 to 1
- point_index: int32 [32], replicated, may hold values from 0 to 63
- w_reduce: bfloat16 [3, 1024, 256], P(None, 'point'), may hold values from -1 to 1
- w_spatial: bfloat16 [3, 2304, 256], P(None, 'point'), may hold values from -0.125 to 0.125
- w_expand: bfloat16 [3, 256, 1024], P(None, 'point'), may hold values from -0.375 to 0.375
- w_classes: bfloat16 [3, 1000, 1024], P(None, None, 'point'), may hold values from -0.1875 to 0.1875
- norm_gain: float32 [3, 1536], replicated, may hold values from 0.5 to 1.5
- norm_bias: float32 [3, 1536], replicated, may hold values from -3 to 3
- class_bias: float32 [3, 1000], replicated, may hold values from -3 to 3
Outputs:
- mean_reduce: float32 [32, 256], P('point')
- var_reduce: float32 [32, 256], P('point')
- mean_spatial: float32 [32, 256], P('point')
- var_spatial: float32 [32, 256], P('point')
- mean_expand: float32 [32, 1024], P('point')
- var_expand: float32 [32, 1024], P('point')
- margin: float32 [32], replicated
The draws below stay inside these ranges and needn't reach their ends.
All inputs are finite; a program needn't handle non-finite values.
Results may differ from the reference program's by a relative error of at most 0.003.
Values may be sent and summed in bfloat16 or wider, within the bound.
No kernel may reach another device: no remote copies, remote signals or barrier semaphores. Data moves between devices by JAX's collectives and lax.ppermute only.
A program may use at most 128 MiB of HBM per device.

```python
import jax
import jax.numpy as jnp
from jax import lax

CIN = 1024
MID = 256
CLASSES = 1000
SIDE = 14
TVALS = 64
NPOINTS = 32
IMGS = 128


def draw_activations(key, part):
    base_key, jitter_key = jax.random.split(key, 2)
    positions = jnp.arange(IMGS, dtype=jnp.float32) / max(IMGS - 1, 1)
    ramp_up = 3.0 ** positions
    jitter = jnp.exp(jax.random.uniform(jitter_key, (IMGS,), jnp.float32, -0.8, 0.8))
    values = jax.random.normal(base_key, (IMGS, SIDE, SIDE, CIN), jnp.float32)
    scales = (0.5 * ramp_up * jitter)[:, None, None, None]
    return jnp.clip(values * scales, -8.0, 8.0).astype(jnp.bfloat16)


def bend_ratio(key):
    return jax.random.uniform(jax.random.fold_in(key, 4242), (), jnp.float32, 0.9, 1.6)


def draw_w_reduce(key, part):
    ratio = bend_ratio(key)
    start_key, final_key = jax.random.split(jax.random.fold_in(key, 1717), 2)
    scale = CIN ** (-0.5)
    start = jnp.clip(jax.random.normal(start_key, (CIN, MID), jnp.float32), -3.0, 3.0) * scale
    final = jnp.clip(jax.random.normal(final_key, (CIN, MID), jnp.float32), -3.0, 3.0) * scale
    bend = -ratio * start
    return jnp.stack([start, bend, final], axis=0).astype(jnp.bfloat16)


def draw_t_values(key, part):
    ratio = bend_ratio(key)
    centre = 0.5 / (1.0 + ratio)
    drawn_key, near_key, pick_key = jax.random.split(jax.random.fold_in(key, 2929), 3)
    width = 0.0015
    drawn = jax.random.uniform(drawn_key, (TVALS,), jnp.float32, 0.0, 1.0)
    near = centre + jax.random.uniform(near_key, (TVALS,), jnp.float32, -width, width)
    picked = jax.random.permutation(pick_key, TVALS) < TVALS // 4
    return jnp.where(picked, near, drawn).astype(jnp.float32)


def set_ends(array, stream_key, low, largest):
    longest = array.shape.index(max(array.shape))
    spots = []
    for shift in (0, 1):
        where = [jax.random.randint(jax.random.fold_in(stream_key, axis), (), 0, length) for axis, length in enumerate(array.shape)]
        where[longest] = (where[longest] + shift) % array.shape[longest]
        spots.append(tuple(where))
    return array.at[spots[0]].set(low).at[spots[1]].set(largest)


def levels(rng, shape, cuts, low, top_value):
    gain = 1.0
    for position, shards_of in cuts:
        steps = jax.random.uniform(jax.random.fold_in(jax.random.fold_in(rng, 6), position), (shards_of,), jnp.float32, low / len(cuts), top_value / len(cuts))
        gain = gain * jnp.repeat(jnp.exp(steps), shape[position] // shards_of).reshape((-1,) + (1,) * (len(shape) - 1 - position))
    return gain


def noise(key, dims, scale, bound, shards=(), kind=jnp.bfloat16):
    result = jax.random.normal(key, dims, jnp.float32) * scale
    if len(shards) > 0:
        result = levels(key, dims, shards, -0.22, 0.18) * result
    return jnp.clip(result, min=-bound, max=bound).astype(kind)


def setup_inputs(seed: int = 0) -> dict:
    seeds = jax.random.split(jax.random.key(seed), 12)
    return {
        "activations": draw_activations(jax.random.fold_in(seeds[11], 71), 0),
        "labels": set_ends(jax.random.randint(seeds[1], (IMGS,), 0, CLASSES), jax.random.fold_in(seeds[1], 1), 0, CLASSES - 1).astype(jnp.int32),
        "t_values": draw_t_values(jax.random.fold_in(seeds[11], 71), 0),
        "point_index": set_ends(jax.random.randint(seeds[3], (NPOINTS,), 0, TVALS), jax.random.fold_in(seeds[3], 1), 0, TVALS - 1).astype(jnp.int32),
        "w_reduce": draw_w_reduce(jax.random.fold_in(seeds[11], 71), 0),
        "w_spatial": noise(seeds[5], (3, 9 * MID, MID), (9 * MID) ** -0.5, 0.125, ((1, 32),)),
        "w_expand": noise(seeds[6], (3, MID, CIN), MID ** -0.5, 0.375, ((1, 32),)),
        "w_classes": noise(seeds[7], (3, CLASSES, CIN), CIN ** -0.5, 0.1875, ((2, 32),)),
        "norm_gain": jnp.clip(jax.random.uniform(seeds[8], (3, 2 * MID + CIN), jnp.float32, 0.5, 1.5), 0.5, 1.5),
        "norm_bias": noise(seeds[9], (3, 2 * MID + CIN), 0.5, 3.0, (), jnp.float32),
        "class_bias": noise(seeds[10], (3, CLASSES), 0.5, 3.0, (), jnp.float32),
    }


EPSILON = 1e-05

def curve_coefficients(t_values, point_index):
    table_size = t_values.shape[0]
    matches = point_index[:, None] == jnp.arange(table_size, dtype=jnp.int32)[None, :]
    picked = lax.optimization_barrier(jnp.sum(jnp.where(matches, t_values[None, :], 0.0), axis=1))
    doubled = 2.0 * picked
    return jnp.stack([jnp.maximum(1.0 - doubled, 0.0), 1.0 - jnp.abs(1.0 - doubled), jnp.maximum(doubled - 1.0, 0.0)], axis=1)

def blend_all(coefficients, endpoints):
    target_shape = (coefficients.shape[0],) + (1,) * (endpoints.ndim - 1)
    start_part = coefficients[:, 0].reshape(target_shape) * endpoints[0].astype(jnp.float32)[None]
    bend_part = coefficients[:, 1].reshape(target_shape) * endpoints[1].astype(jnp.float32)[None]
    final_part = coefficients[:, 2].reshape(target_shape) * endpoints[2].astype(jnp.float32)[None]
    return start_part + bend_part + final_part

def normalize(pre_norm, gain_part, bias_part):
    channel_mean = lax.optimization_barrier(jnp.mean(pre_norm, axis=0))
    channel_var = lax.optimization_barrier(jnp.mean(jnp.square(pre_norm - channel_mean), axis=0))
    scaled = (pre_norm - channel_mean) * lax.rsqrt(channel_var + EPSILON) * gain_part + bias_part
    return (channel_mean, channel_var, scaled)

def spatial_conv(source, kernel):
    images, side_len, _, middle = source.shape
    padded = jnp.pad(source, ((0, 0), (1, 1), (1, 1), (0, 0)))
    summed = jnp.zeros((images * side_len * side_len, kernel.shape[1]), jnp.float32)
    for offset in range(9):
        shift_y, shift_x = (offset // 3, offset % 3)
        window = padded[:, shift_y:shift_y + side_len, shift_x:shift_x + side_len, :].reshape(images * side_len * side_len, middle)
        summed = summed + jnp.dot(window, kernel[offset * middle:(offset + 1) * middle], preferred_element_type=jnp.float32)
    return summed

def reference(activations, labels, t_values, point_index, w_reduce, w_spatial, w_expand, w_classes, norm_gain, norm_bias, class_bias):
    coefficients = curve_coefficients(t_values, point_index)
    flattened = activations.reshape(IMGS * SIDE * SIDE, CIN)
    onehot = labels[:, None] == jnp.arange(CLASSES, dtype=jnp.int32)[None, :]

    def one_point(coefficient_row):
        own_row = coefficient_row.reshape(1, 3)
        reduce_w = blend_all(own_row, w_reduce)[0].astype(jnp.bfloat16)
        spatial_w = blend_all(own_row, w_spatial)[0].astype(jnp.bfloat16)
        expand_w = blend_all(own_row, w_expand)[0].astype(jnp.bfloat16)
        class_w = blend_all(own_row, w_classes)[0].astype(jnp.bfloat16)
        gain_now = blend_all(own_row, norm_gain)[0]
        bias_now = blend_all(own_row, norm_bias)[0]
        shift_now = blend_all(own_row, class_bias)[0]
        reduced = jnp.dot(flattened, reduce_w, preferred_element_type=jnp.float32)
        mean_one, var_one, normed_one = normalize(reduced, gain_now[:MID], bias_now[:MID])
        first = jax.nn.relu(normed_one).astype(jnp.bfloat16).reshape(IMGS, SIDE, SIDE, MID)
        spatial = spatial_conv(first, spatial_w)
        mean_two, var_two, normed_two = normalize(spatial, gain_now[MID:2 * MID], bias_now[MID:2 * MID])
        second = jax.nn.relu(normed_two).astype(jnp.bfloat16)
        expanded = jnp.dot(second, expand_w, preferred_element_type=jnp.float32)
        mean_three, var_three, normed_three = normalize(expanded, gain_now[2 * MID:], bias_now[2 * MID:])
        block_out = jax.nn.relu(normed_three + flattened.astype(jnp.float32))
        pooled = lax.optimization_barrier(jnp.mean(block_out.reshape(IMGS, SIDE * SIDE, CIN), axis=1)).astype(jnp.bfloat16)
        logits = lax.dot_general(pooled, class_w, (((1,), (1,)), ((), ())), preferred_element_type=jnp.float32) + shift_now
        correct = lax.optimization_barrier(jnp.sum(jnp.where(onehot, logits, 0.0), axis=1))
        rivals = lax.optimization_barrier(jnp.max(jnp.where(onehot, -1e+30, logits), axis=1))
        margin_value = jnp.sum(correct - rivals) / IMGS
        return (mean_one, var_one, mean_two, var_two, mean_three, var_three, margin_value)
    results = lax.map(one_point, coefficients)
    return (results[0], results[1], results[2], results[3], results[4], results[5], results[6])
```

```python
import jax
import jax.numpy as jnp
from jax import lax
from jax.experimental import pallas as pl
from jax.experimental.pallas import tpu as pltpu
from jax.sharding import Mesh
from jax.sharding import PartitionSpec as P

POINT = ("pz", "px", "py")
BATCH = ("bz", "core")
EPSILON = 1e-05
SM = pl.BlockSpec(memory_space=pltpu.SMEM)
VM = pl.BlockSpec(memory_space=pltpu.VMEM)
HBM = pl.BlockSpec(memory_space=pltpu.HBM)


def coefficients_of(values_ref, index_ref, point):
    doubled = 2.0 * values_ref[index_ref[point]]
    return (
        jnp.maximum(1.0 - doubled, 0.0),
        1.0 - jnp.abs(1.0 - doubled),
        jnp.maximum(doubled - 1.0, 0.0),
    )


def blend(row, parts):
    return row[0] * parts[0] + row[1] * parts[1] + row[2] * parts[2]


def first_weights(t_values, point_index, own, w_reduce, gains, biases, class_bias, lanes):
    _, rows, middle = w_reduce.shape
    points = point_index.shape[0]
    classes = class_bias.shape[1]

    def body(values_ref, index_ref, own_ref, reduce_ref, gains_ref, biases_ref, class_ref,
             out_ref, gain_ref, bias_ref, shift_ref, wide_ref):
        wide_ref[...] = reduce_ref[...].astype(jnp.float32)

        def one(point, carry):
            row = coefficients_of(values_ref, index_ref, point)
            out_ref[point] = blend(row, wide_ref).astype(jnp.bfloat16)
            return carry

        lax.fori_loop(0, points, one, 0)
        row = coefficients_of(values_ref, index_ref, own_ref[0])

        def ends(ref):
            return [ref[k : k + 1, :] for k in range(3)]

        gain_ref[...] = blend(row, ends(gains_ref))
        bias_ref[...] = blend(row, ends(biases_ref))
        shift_ref[...] = jnp.full((1, lanes), -1e30, jnp.float32)
        shift_ref[:, :classes] = blend(row, ends(class_ref))

    return pl.pallas_call(
        body,
        name="first_weights",
        in_specs=[SM, SM, SM, VM, VM, VM, VM],
        out_specs=[VM] * 4,
        out_shape=[
            jax.ShapeDtypeStruct((points, rows, middle), jnp.bfloat16),
            jax.ShapeDtypeStruct((1, gains.shape[1]), jnp.float32),
            jax.ShapeDtypeStruct((1, biases.shape[1]), jnp.float32),
            jax.ShapeDtypeStruct((1, lanes), jnp.float32),
        ],
        scratch_shapes=[pltpu.VMEM(w_reduce.shape, jnp.float32)],
        compiler_params=pltpu.CompilerParams(vmem_limit_bytes=16 << 20),
    )(t_values, point_index, own, w_reduce, gains, biases, class_bias)


def other_weights(t_values, point_index, w_spatial, w_expand, w_classes, lanes):
    _, taps, middle = w_spatial.shape
    _, rows, channels = w_expand.shape
    _, cols, classes = w_classes.shape
    points = point_index.shape[0]
    pieces = channels // middle
    packed = taps + pieces * rows

    def body(values_ref, index_ref, spatial_ref, expand_ref, classes_ref, conv_ref, class_ref,
             packed_ref, wide_ref):
        packed_ref[:, :taps, :] = spatial_ref[...].astype(jnp.float32)
        for piece in range(pieces):
            start = taps + piece * rows
            packed_ref[:, start : start + rows, :] = expand_ref[
                :, :, piece * middle : (piece + 1) * middle
            ].astype(jnp.float32)
        wide_ref[...] = jnp.zeros(wide_ref.shape, jnp.float32)
        wide_ref[:, :, :classes] = classes_ref[...].astype(jnp.float32)

        def one(point, carry):
            row = coefficients_of(values_ref, index_ref, point)
            conv_ref[point] = blend(row, packed_ref).astype(jnp.bfloat16)
            class_ref[point] = blend(row, wide_ref).astype(jnp.bfloat16)
            return carry

        lax.fori_loop(0, points, one, 0)

    return pl.pallas_call(
        body,
        name="other_weights",
        in_specs=[SM, SM, VM, VM, VM],
        out_specs=[VM] * 2,
        out_shape=[
            jax.ShapeDtypeStruct((points, packed, middle), jnp.bfloat16),
            jax.ShapeDtypeStruct((points, cols, lanes), jnp.bfloat16),
        ],
        scratch_shapes=[
            pltpu.VMEM((3, packed, middle), jnp.float32),
            pltpu.VMEM((3, cols, lanes), jnp.float32),
        ],
        compiler_params=pltpu.CompilerParams(vmem_limit_bytes=16 << 20),
    )(t_values, point_index, w_spatial, w_expand, w_classes)


def exchange(x):
    return lax.all_to_all(x, POINT, split_axis=0, concat_axis=0, tiled=True)


def batch_sum(x):
    x = x + lax.ppermute(x, "core", [(0, 1), (1, 0)])
    return x + lax.ppermute(x, "bz", [(0, 1), (1, 0)])


def cost(flops):
    return pl.CostEstimate(flops=flops, transcendentals=0, bytes_accessed=flops // 512)


def column_sums(x):
    return jnp.sum(x.reshape(x.shape[0] // 8, 8, x.shape[1]), axis=0)


def moments(sums, rows):
    mean = sums[0:1] * (1.0 / rows)
    var = sums[1:2] * (1.0 / rows) - mean * mean
    return mean, var


def reduce_stage(maps, weight, side, images):
    rows, channels = maps.shape
    middle = weight.shape[1]
    chunk = side * images

    def body(maps_ref, weight_ref, reduced_ref, sums_ref, held_ref, block_ref, sems, out_sems):
        def copy(step):
            part = pl.ds(step * chunk, chunk)
            return pltpu.make_async_copy(maps_ref.at[part], held_ref.at[part], sems.at[step])

        def copy_out(step):
            part = pl.ds(step * chunk, chunk)
            return pltpu.make_async_copy(
                block_ref.at[part], reduced_ref.at[part], out_sems.at[step]
            )

        for step in range(side):
            copy(step).start()

        def one(step, carry):
            total, squares = carry
            copy(step).wait()
            part = pl.ds(step * chunk, chunk)
            product = jnp.dot(
                held_ref[part, :], weight_ref[...], preferred_element_type=jnp.float32
            )
            block_ref[part, :] = product
            copy_out(step).start()
            return total + column_sums(product), squares + column_sums(product * product)

        zero = jnp.zeros((8, middle), jnp.float32)
        total, squares = lax.fori_loop(0, side, one, (zero, zero))
        sums_ref[0:1, :] = jnp.sum(total, axis=0, keepdims=True)
        sums_ref[1:2, :] = jnp.sum(squares, axis=0, keepdims=True)
        for step in range(side):
            copy_out(step).wait()

    return pl.pallas_call(
        body,
        name="reduce_stage",
        in_specs=[HBM, VM],
        out_specs=[HBM, VM],
        out_shape=[
            pltpu.HBM((rows, middle), jnp.float32),
            jax.ShapeDtypeStruct((2, middle), jnp.float32),
        ],
        scratch_shapes=[
            pltpu.VMEM((rows, channels), jnp.bfloat16),
            pltpu.VMEM((rows, middle), jnp.float32),
            pltpu.SemaphoreType.DMA((side,)),
            pltpu.SemaphoreType.DMA((side,)),
        ],
        compiler_params=pltpu.CompilerParams(vmem_limit_bytes=32 << 20),
        cost_estimate=cost(2 * rows * channels * middle),
    )(maps, weight)


def spatial_stage(reduced, sums, gain, bias, weights, taps, side, images, row_count):
    rows, middle = reduced.shape
    shards_of, packed, _ = weights.shape
    mixed = shards_of * taps
    pieces = 4
    each = (packed - taps) // pieces
    chunk = side * images
    wide = chunk + 2 * images

    def body(reduced_ref, sums_ref, gain_ref, bias_ref, weights_ref, spatial_ref, out_ref,
             mean_ref, var_ref, expand_ref, first_ref, weight_ref, held_ref, sems):
        def copy(step):
            part = pl.ds(step * chunk, chunk)
            return pltpu.make_async_copy(reduced_ref.at[part], held_ref.at[part], sems.at[step])

        for step in range(side):
            copy(step).start()
        mean, var = moments(sums_ref[...], row_count)
        mean_ref[...] = mean
        var_ref[...] = var
        scale = lax.rsqrt(var + EPSILON) * gain_ref[...]
        shift = bias_ref[...] - mean * scale
        weight_ref[...] = (
            weights_ref[:, :taps, :]
            .astype(jnp.float32)
            .reshape(mixed, middle)
            .astype(jnp.bfloat16)
        )
        for piece in range(pieces):
            start = taps + piece * each
            expand_ref[:, piece * middle : (piece + 1) * middle] = (
                weights_ref[:, start : start + each, :]
                .astype(jnp.float32)
                .reshape(shards_of * each, middle)
                .astype(jnp.bfloat16)
            )
        edge = jnp.zeros((images, middle), jnp.bfloat16)
        first_ref[0] = jnp.zeros((wide, middle), jnp.bfloat16)
        first_ref[side + 1] = jnp.zeros((wide, middle), jnp.bfloat16)

        def norm(row, carry):
            copy(row).wait()
            values = held_ref[pl.ds(row * chunk, chunk), :]
            values = jnp.maximum(values * scale + shift, 0.0)
            first_ref[row + 1, 0:images, :] = edge
            first_ref[row + 1, images : images + chunk, :] = values.astype(jnp.bfloat16)
            first_ref[row + 1, images + chunk :, :] = edge
            return carry

        lax.fori_loop(0, side, norm, 0)

        def one(step, carry):
            total, squares = carry
            windows = [
                first_ref[step + dy, dx * images : dx * images + chunk, :]
                for dy in range(3)
                for dx in range(3)
            ]
            product = sum(
                jnp.dot(
                    window,
                    weight_ref[tap * middle : (tap + 1) * middle, :],
                    preferred_element_type=jnp.float32,
                )
                for tap, window in enumerate(windows)
            )
            spatial_ref[pl.ds(step * chunk, chunk), :] = product
            return total + column_sums(product), squares + column_sums(product * product)

        zero = jnp.zeros((8, middle), jnp.float32)
        total, squares = lax.fori_loop(0, side, one, (zero, zero))
        out_ref[0:1, :] = jnp.sum(total, axis=0, keepdims=True)
        out_ref[1:2, :] = jnp.sum(squares, axis=0, keepdims=True)

    return pl.pallas_call(
        body,
        name="spatial_stage",
        in_specs=[HBM] + [VM] * 4,
        out_specs=[VM] * 5,
        out_shape=[
            jax.ShapeDtypeStruct((rows, middle), jnp.float32),
            jax.ShapeDtypeStruct((2, middle), jnp.float32),
            jax.ShapeDtypeStruct((1, middle), jnp.float32),
            jax.ShapeDtypeStruct((1, middle), jnp.float32),
            jax.ShapeDtypeStruct((shards_of * each, pieces * middle), jnp.bfloat16),
        ],
        scratch_shapes=[
            pltpu.VMEM((side + 2, wide, middle), jnp.bfloat16),
            pltpu.VMEM((mixed, middle), jnp.bfloat16),
            pltpu.VMEM((rows, middle), jnp.float32),
            pltpu.SemaphoreType.DMA((side,)),
        ],
        compiler_params=pltpu.CompilerParams(vmem_limit_bytes=24 << 20),
        cost_estimate=cost(2 * rows * mixed * middle),
    )(reduced, sums, gain, bias, weights)


def second_stage(spatial, sums, gain, bias, weight, side, images, row_count):
    rows, middle = spatial.shape
    channels = weight.shape[1]
    chunk = side * images

    def body(spatial_ref, sums_ref, gain_ref, bias_ref, weight_ref, second_ref, out_ref,
             mean_ref, var_ref):
        mean, var = moments(sums_ref[...], row_count)
        mean_ref[...] = mean
        var_ref[...] = var
        scale = lax.rsqrt(var + EPSILON) * gain_ref[...]
        shift = bias_ref[...] - mean * scale

        def one(step, carry):
            total, gram = carry
            part = pl.ds(step * chunk, chunk)
            values = jnp.maximum(spatial_ref[part, :] * scale + shift, 0.0).astype(jnp.bfloat16)
            second_ref[part, :] = values
            gram = gram + lax.dot_general(
                values, values, (((0,), (0,)), ((), ())), preferred_element_type=jnp.float32
            )
            return total + column_sums(values.astype(jnp.float32)), gram

        total, gram = lax.fori_loop(
            0,
            side,
            one,
            (jnp.zeros((8, middle), jnp.float32), jnp.zeros((middle, middle), jnp.float32)),
        )
        stacked = jnp.concatenate([gram, total], axis=0)
        high = stacked.astype(jnp.bfloat16)
        rest = stacked - high.astype(jnp.float32)
        mid = rest.astype(jnp.bfloat16)
        low = (rest - mid.astype(jnp.float32)).astype(jnp.bfloat16)
        kernel = weight_ref[...]
        product = (
            jnp.dot(low, kernel, preferred_element_type=jnp.float32)
            + jnp.dot(mid, kernel, preferred_element_type=jnp.float32)
            + jnp.dot(high, kernel, preferred_element_type=jnp.float32)
        )
        out_ref[0:1, :] = jnp.sum(product[middle:], axis=0, keepdims=True)
        out_ref[1:2, :] = jnp.sum(
            product[:middle] * kernel.astype(jnp.float32), axis=0, keepdims=True
        )

    return pl.pallas_call(
        body,
        name="second_stage",
        in_specs=[VM] * 5,
        out_specs=[VM] * 4,
        out_shape=[
            jax.ShapeDtypeStruct((rows, middle), jnp.bfloat16),
            jax.ShapeDtypeStruct((2, channels), jnp.float32),
            jax.ShapeDtypeStruct((1, middle), jnp.float32),
            jax.ShapeDtypeStruct((1, middle), jnp.float32),
        ],
        compiler_params=pltpu.CompilerParams(vmem_limit_bytes=16 << 20),
        cost_estimate=cost(2 * rows * middle * middle),
    )(spatial, sums, gain, bias, weight)


def output_stage(second, maps, sums, gain, bias, weight, side, images, row_count):
    rows, middle = second.shape
    channels = weight.shape[1]
    chunk = side * images
    tiles = 4
    width = channels // tiles

    def body(second_ref, maps_ref, sums_ref, gain_ref, bias_ref, weight_ref, out_ref, mean_ref,
             var_ref, pooled_ref, held_ref, sems):
        def copy(step):
            part = pl.ds(step * chunk, chunk)
            return pltpu.make_async_copy(maps_ref.at[part], held_ref.at[part], sems.at[step])

        for step in range(side):
            copy(step).start()
        mean, var = moments(sums_ref[...], row_count)
        mean_ref[...] = mean
        var_ref[...] = var
        scale_all = lax.rsqrt(var + EPSILON) * gain_ref[...]
        shift_all = bias_ref[...] - mean * scale_all
        pooled_ref[...] = jnp.zeros((images, channels), jnp.float32)

        def one(step, carry):
            copy(step).wait()
            part = pl.ds(step * chunk, chunk)
            for tile in range(tiles):
                cols = slice(tile * width, (tile + 1) * width)
                product = jnp.dot(
                    second_ref[part, :], weight_ref[:, cols], preferred_element_type=jnp.float32
                )
                values = product * scale_all[:, cols] + (
                    shift_all[:, cols] + held_ref[part, cols].astype(jnp.float32)
                )
                values = jnp.maximum(values, 0.0)
                pooled_ref[:, cols] += jnp.sum(values.reshape(side, images, width), axis=0)
            return carry

        lax.fori_loop(0, side, one, 0)
        out_ref[...] = (pooled_ref[...] * (1.0 / (side * side))).astype(jnp.bfloat16)

    return pl.pallas_call(
        body,
        name="output_stage",
        in_specs=[VM, HBM] + [VM] * 4,
        out_specs=[VM] * 3,
        out_shape=[
            jax.ShapeDtypeStruct((images, channels), jnp.bfloat16),
            jax.ShapeDtypeStruct((1, channels), jnp.float32),
            jax.ShapeDtypeStruct((1, channels), jnp.float32),
        ],
        scratch_shapes=[
            pltpu.VMEM((images, channels), jnp.float32),
            pltpu.VMEM((rows, channels), jnp.bfloat16),
            pltpu.SemaphoreType.DMA((side,)),
        ],
        compiler_params=pltpu.CompilerParams(vmem_limit_bytes=24 << 20),
        cost_estimate=cost(2 * rows * channels * middle),
    )(second, maps, sums, gain, bias, weight)


def probe_stage(pooled, class_w, shift, labels, image_count):
    images, channels = pooled.shape
    lanes = class_w.shape[1]

    def body(labels_ref, pooled_ref, class_ref, shift_ref, margin_ref):
        logits = (
            jnp.dot(pooled_ref[...], class_ref[...], preferred_element_type=jnp.float32)
            + shift_ref[...]
        )
        index = lax.broadcasted_iota(jnp.int32, (images, 1), 0)
        column = jnp.zeros((images, 1), jnp.int32)
        for image in range(images):
            column = jnp.where(index == image, labels_ref[image], column)
        onehot = lax.broadcasted_iota(jnp.int32, (images, lanes), 1) == column
        correct = jnp.sum(jnp.where(onehot, logits, 0.0), axis=1, keepdims=True)
        rivals = jnp.max(jnp.where(onehot, -1e30, logits), axis=1, keepdims=True)
        total = jnp.sum(correct - rivals, axis=0, keepdims=True) * (1.0 / image_count)
        margin_ref[...] = jnp.broadcast_to(total, (1, 128))

    return pl.pallas_call(
        body,
        name="probe_stage",
        in_specs=[SM, VM, VM, VM],
        out_specs=VM,
        out_shape=jax.ShapeDtypeStruct((1, 128), jnp.float32),
        compiler_params=pltpu.CompilerParams(vmem_limit_bytes=8 << 20),
    )(labels, pooled, class_w, shift)


def shards(activations, labels, t_values, point_index, w_reduce, w_spatial, w_expand, w_classes,
           norm_gain, norm_bias, class_bias):
    images, side, _, channels = activations.shape
    middle = w_reduce.shape[2]
    image_count = images * lax.axis_size(BATCH)
    row_count = float(image_count * side * side)
    lanes = -(-class_bias.shape[1] // 128) * 128
    own = jnp.reshape(lax.axis_index(POINT), (1,)).astype(jnp.int32)
    sent, gain, bias, shift = first_weights(
        t_values, point_index, own, w_reduce, norm_gain, norm_bias, class_bias, lanes
    )
    reduce_w = exchange(sent).reshape(channels, middle)
    packed, class_sent = other_weights(
        t_values, point_index, w_spatial, w_expand, jnp.swapaxes(w_classes, 1, 2), lanes
    )
    packed, reduce_w = lax.optimization_barrier((packed, reduce_w))
    weights = exchange(packed)
    maps = jnp.transpose(activations, (1, 2, 0, 3)).reshape(side * side * images, channels)
    maps = pltpu.with_memory_space_constraint(maps, pltpu.HBM)
    reduced, sums = reduce_stage(maps, reduce_w, side, images)
    class_sent, sums = lax.optimization_barrier((class_sent, sums))
    class_w = exchange(class_sent).reshape(channels, lanes)
    sums = batch_sum(sums)
    reduced = pltpu.with_memory_space_constraint(reduced, pltpu.HBM)
    spatial, sums, mean_one, var_one, expand_w = spatial_stage(
        reduced, sums, gain[:, :middle], bias[:, :middle], weights, w_spatial.shape[1], side,
        images, row_count
    )
    sums = batch_sum(sums)
    second, sums, mean_two, var_two = second_stage(
        spatial, sums, gain[:, middle : 2 * middle], bias[:, middle : 2 * middle], expand_w,
        side, images, row_count
    )
    sums = batch_sum(sums)
    pooled, mean_three, var_three = output_stage(
        second, maps, sums, gain[:, 2 * middle :], bias[:, 2 * middle :], expand_w, side, images,
        row_count
    )
    margin = probe_stage(pooled, class_w, shift, labels, image_count)
    margin = batch_sum(margin)
    points = lax.axis_size(POINT)
    copies = jnp.broadcast_to(margin[None], (points, 1, 128))
    margin_all = exchange(copies)[:, 0, 0]
    return mean_one, var_one, mean_two, var_two, mean_three, var_three, margin_all


def solution(mesh):
    torus = Mesh(mesh.devices.reshape(2, 4, 4, 2, 2), POINT + BATCH)
    rows = P(POINT, None)
    return jax.shard_map(
        shards,
        mesh=torus,
        in_specs=(
            P(BATCH, None, None, None),
            P(BATCH),
            P(),
            P(),
            P(None, POINT, None),
            P(None, POINT, None),
            P(None, POINT, None),
            P(None, None, POINT),
            P(),
            P(),
            P(),
        ),
        out_specs=(rows, rows, rows, rows, rows, rows, P()),
        check_vma=False,
    )
```

```python
import jax
import jax.numpy as jnp
from jax import lax
from jax.experimental import pallas as pl
from jax.experimental.pallas import tpu as pltpu
from jax.sharding import Mesh
from jax.sharding import PartitionSpec as P

POINT = ("pz", "px", "py")
BATCH = ("bz", "core")
EPSILON = 1e-05
SM = pl.BlockSpec(memory_space=pltpu.SMEM)
VM = pl.BlockSpec(memory_space=pltpu.VMEM)
HBM = pl.BlockSpec(memory_space=pltpu.HBM)


def coefficients_of(values_ref, index_ref, point):
    doubled = 2.0 * values_ref[index_ref[point]]
    return (
        jnp.maximum(1.0 - doubled, 0.0),
        1.0 - jnp.abs(1.0 - doubled),
        jnp.maximum(doubled - 1.0, 0.0),
    )


def blend(row, parts):
    return row[0] * parts[0] + row[1] * parts[1] + row[2] * parts[2]


def fetch(pairs, sems):
    copies = [
        pltpu.make_async_copy(source, target, sems.at[k])
        for k, (source, target) in enumerate(pairs)
    ]
    for copy in copies:
        copy.start()
    for copy in copies:
        copy.wait()


def in_hbm(*arrays):
    return [pltpu.with_memory_space_constraint(x, pltpu.HBM) for x in arrays]


def first_weights(t_values, point_index, own, w_reduce, gains, biases, class_bias, lanes):
    _, rows, middle = w_reduce.shape
    points = point_index.shape[0]
    classes = class_bias.shape[1]

    def body(own_ref, *refs):
        sources = refs[:6]
        out_ref, gain_ref, bias_ref, shift_ref = refs[6:10]
        values_ref, index_ref, reduce_ref, gains_ref, biases_ref, class_ref = refs[10:16]
        wide_ref, sems = refs[16:]
        fetch(list(zip(sources, refs[10:16])), sems)
        wide_ref[...] = reduce_ref[...].astype(jnp.float32)

        def one(point, carry):
            row = coefficients_of(values_ref, index_ref, point)
            out_ref[point] = blend(row, wide_ref).astype(jnp.bfloat16)
            return carry

        lax.fori_loop(0, points, one, 0)
        row = coefficients_of(values_ref, index_ref, own_ref[0])

        def ends(ref):
            return [ref[k : k + 1, :] for k in range(3)]

        gain_ref[...] = blend(row, ends(gains_ref))
        bias_ref[...] = blend(row, ends(biases_ref))
        shift_ref[...] = jnp.full((1, lanes), -1e30, jnp.float32)
        shift_ref[:, :classes] = blend(row, ends(class_ref))

    return pl.pallas_call(
        body,
        name="first_weights",
        in_specs=[SM] + [HBM] * 6,
        out_specs=[VM] * 4,
        out_shape=[
            jax.ShapeDtypeStruct((points, rows, middle), jnp.bfloat16),
            jax.ShapeDtypeStruct((1, gains.shape[1]), jnp.float32),
            jax.ShapeDtypeStruct((1, biases.shape[1]), jnp.float32),
            jax.ShapeDtypeStruct((1, lanes), jnp.float32),
        ],
        scratch_shapes=[
            pltpu.SMEM(t_values.shape, jnp.float32),
            pltpu.SMEM(point_index.shape, jnp.int32),
            pltpu.VMEM(w_reduce.shape, w_reduce.dtype),
            pltpu.VMEM(gains.shape, jnp.float32),
            pltpu.VMEM(biases.shape, jnp.float32),
            pltpu.VMEM(class_bias.shape, jnp.float32),
            pltpu.VMEM(w_reduce.shape, jnp.float32),
            pltpu.SemaphoreType.DMA((6,)),
        ],
        compiler_params=pltpu.CompilerParams(vmem_limit_bytes=16 << 20),
    )(own, *in_hbm(t_values, point_index, w_reduce, gains, biases, class_bias))


def other_weights(t_values, point_index, own, w_spatial, w_expand, w_classes, lanes):
    _, taps, middle = w_spatial.shape
    _, rows, channels = w_expand.shape
    _, cols, classes = w_classes.shape
    points = point_index.shape[0]
    lane = middle // 2
    tiles = channels // (2 * lane)
    class_tiles = lanes // (2 * lane)
    conv_rows = taps + tiles * rows
    packed = conv_rows + class_tiles * cols
    groups = 4
    each = points // groups

    def body(own_ref, values_in, index_in, spatial_in, expand_in, classes_in, out_ref,
             values_ref, index_ref, spatial_ref, expand_ref, classes_ref, packed_ref, wide_ref,
             block_ref, sems, out_sems):
        fetch(
            [
                (values_in, values_ref),
                (index_in, index_ref),
                (spatial_in, spatial_ref),
                (expand_in, expand_ref),
                (classes_in, classes_ref),
            ],
            sems,
        )
        low = own_ref[1] == 0
        wide_ref[...] = jnp.zeros(wide_ref.shape, jnp.float32)
        wide_ref[:, :, :classes] = classes_ref[...].astype(jnp.float32)

        def half(ref, tile, tiles_of):
            first = ref[:, :, tile * lane : (tile + 1) * lane].astype(jnp.float32)
            start = (tiles_of + tile) * lane
            last = ref[:, :, start : start + lane].astype(jnp.float32)
            return jnp.where(low, first, last)

        packed_ref[:, :taps, :] = half(spatial_ref, 0, 1)
        for tile in range(tiles):
            start = taps + tile * rows
            packed_ref[:, start : start + rows, :] = half(expand_ref, tile, tiles)
        for tile in range(class_tiles):
            start = conv_rows + tile * cols
            packed_ref[:, start : start + cols, :] = half(wide_ref, tile, class_tiles)

        def copy_out(group):
            part = pl.ds(group * each, each)
            return pltpu.make_async_copy(
                block_ref.at[part], out_ref.at[part], out_sems.at[group]
            )

        def one(point, carry):
            row = coefficients_of(values_ref, index_ref, point)
            block_ref[point] = blend(row, packed_ref).astype(jnp.bfloat16)
            return carry

        for group in range(groups):
            lax.fori_loop(group * each, (group + 1) * each, one, 0)
            copy_out(group).start()
        for group in range(groups):
            copy_out(group).wait()

    return pl.pallas_call(
        body,
        name="other_weights",
        in_specs=[SM] + [HBM] * 5,
        out_specs=HBM,
        out_shape=pltpu.HBM((points, packed, lane), jnp.bfloat16),
        scratch_shapes=[
            pltpu.SMEM(t_values.shape, jnp.float32),
            pltpu.SMEM(point_index.shape, jnp.int32),
            pltpu.VMEM(w_spatial.shape, w_spatial.dtype),
            pltpu.VMEM(w_expand.shape, w_expand.dtype),
            pltpu.VMEM(w_classes.shape, w_classes.dtype),
            pltpu.VMEM((3, packed, lane), jnp.float32),
            pltpu.VMEM((3, cols, lanes), jnp.float32),
            pltpu.VMEM((points, packed, lane), jnp.bfloat16),
            pltpu.SemaphoreType.DMA((5,)),
            pltpu.SemaphoreType.DMA((groups,)),
        ],
        compiler_params=pltpu.CompilerParams(vmem_limit_bytes=16 << 20),
    )(own, *in_hbm(t_values, point_index, w_spatial, w_expand, w_classes))


def exchange(x):
    return lax.all_to_all(x, POINT, split_axis=0, concat_axis=0, tiled=True)


def batch_sum(x):
    x = x + lax.ppermute(x, "core", [(0, 1), (1, 0)])
    return x + lax.ppermute(x, "bz", [(0, 1), (1, 0)])


def cost(flops):
    return pl.CostEstimate(flops=flops, transcendentals=0, bytes_accessed=flops // 512)


def column_sums(x):
    return jnp.sum(x.reshape(x.shape[0] // 8, 8, x.shape[1]), axis=0)


def moments(sums, rows):
    mean = sums[0:1] * (1.0 / rows)
    var = sums[1:2] * (1.0 / rows) - mean * mean
    return mean, var


def reduce_stage(maps, weight, side, images):
    rows, channels = maps.shape
    middle = weight.shape[1]
    chunk = side * images

    def body(maps_ref, weight_ref, reduced_ref, sums_ref, held_ref, block_ref, sems, out_sems):
        def copy(step):
            part = pl.ds(step * chunk, chunk)
            return pltpu.make_async_copy(maps_ref.at[part], held_ref.at[part], sems.at[step])

        def copy_out(step):
            part = pl.ds(step * chunk, chunk)
            return pltpu.make_async_copy(
                block_ref.at[part], reduced_ref.at[part], out_sems.at[step]
            )

        for step in range(side):
            copy(step).start()

        def one(step, carry):
            total, squares = carry
            copy(step).wait()
            part = pl.ds(step * chunk, chunk)
            product = jnp.dot(
                held_ref[part, :], weight_ref[...], preferred_element_type=jnp.float32
            )
            block_ref[part, :] = product
            copy_out(step).start()
            return total + column_sums(product), squares + column_sums(product * product)

        zero = jnp.zeros((8, middle), jnp.float32)
        total, squares = lax.fori_loop(0, side, one, (zero, zero))
        sums_ref[0:1, :] = jnp.sum(total, axis=0, keepdims=True)
        sums_ref[1:2, :] = jnp.sum(squares, axis=0, keepdims=True)
        for step in range(side):
            copy_out(step).wait()

    return pl.pallas_call(
        body,
        name="reduce_stage",
        in_specs=[HBM, VM],
        out_specs=[HBM, VM],
        out_shape=[
            pltpu.HBM((rows, middle), jnp.float32),
            jax.ShapeDtypeStruct((2, middle), jnp.float32),
        ],
        scratch_shapes=[
            pltpu.VMEM((rows, channels), jnp.bfloat16),
            pltpu.VMEM((rows, middle), jnp.float32),
            pltpu.SemaphoreType.DMA((side,)),
            pltpu.SemaphoreType.DMA((side,)),
        ],
        compiler_params=pltpu.CompilerParams(vmem_limit_bytes=32 << 20),
        cost_estimate=cost(2 * rows * channels * middle),
    )(maps, weight)


def spatial_stage(own, reduced, sums, gain, bias, mine, other, taps, expand_rows, side, images,
                  row_count):
    rows, middle = reduced.shape
    shards_of, _, lane = mine.shape
    mixed = shards_of * taps
    pieces = 4
    each = expand_rows
    packed = taps + pieces * each
    chunk = side * images
    wide = chunk + 2 * images

    def body(own_ref, reduced_ref, mine_ref, other_ref, sums_ref, gain_ref, bias_ref,
             spatial_ref, out_ref, mean_ref, var_ref, expand_ref, first_ref, weight_ref, held_ref,
             halves_ref, sems, half_sems):
        core = own_ref[1]
        rows_of = pl.ds(0, packed)
        halves = [
            pltpu.make_async_copy(
                mine_ref.at[:, rows_of, :], halves_ref.at[core], half_sems.at[0]
            ),
            pltpu.make_async_copy(
                other_ref.at[:, rows_of, :], halves_ref.at[1 - core], half_sems.at[1]
            ),
        ]

        def copy(step):
            part = pl.ds(step * chunk, chunk)
            return pltpu.make_async_copy(reduced_ref.at[part], held_ref.at[part], sems.at[step])

        for step in range(side):
            copy(step).start()
        for half in halves:
            half.start()
        mean, var = moments(sums_ref[...], row_count)
        mean_ref[...] = mean
        var_ref[...] = var
        scale = lax.rsqrt(var + EPSILON) * gain_ref[...]
        shift = bias_ref[...] - mean * scale
        edge = jnp.zeros((images, middle), jnp.bfloat16)
        first_ref[0] = jnp.zeros((wide, middle), jnp.bfloat16)
        first_ref[side + 1] = jnp.zeros((wide, middle), jnp.bfloat16)

        def norm(row, carry):
            copy(row).wait()
            values = held_ref[pl.ds(row * chunk, chunk), :]
            values = jnp.maximum(values * scale + shift, 0.0)
            first_ref[row + 1, 0:images, :] = edge
            first_ref[row + 1, images : images + chunk, :] = values.astype(jnp.bfloat16)
            first_ref[row + 1, images + chunk :, :] = edge
            return carry

        lax.fori_loop(0, side, norm, 0)
        for half in halves:
            half.wait()
        for half in range(2):
            weight_ref[:, half * lane : (half + 1) * lane] = (
                halves_ref[half, :, :taps, :]
                .astype(jnp.float32)
                .reshape(mixed, lane)
                .astype(jnp.bfloat16)
            )
            for piece in range(pieces):
                start = taps + piece * each
                column = (half * pieces + piece) * lane
                expand_ref[:, column : column + lane] = (
                    halves_ref[half, :, start : start + each, :]
                    .astype(jnp.float32)
                    .reshape(shards_of * each, lane)
                    .astype(jnp.bfloat16)
                )

        def one(step, carry):
            total, squares = carry
            windows = [
                first_ref[step + dy, dx * images : dx * images + chunk, :]
                for dy in range(3)
                for dx in range(3)
            ]
            product = sum(
                jnp.dot(
                    window,
                    weight_ref[tap * middle : (tap + 1) * middle, :],
                    preferred_element_type=jnp.float32,
                )
                for tap, window in enumerate(windows)
            )
            spatial_ref[pl.ds(step * chunk, chunk), :] = product
            return total + column_sums(product), squares + column_sums(product * product)

        zero = jnp.zeros((8, middle), jnp.float32)
        total, squares = lax.fori_loop(0, side, one, (zero, zero))
        out_ref[0:1, :] = jnp.sum(total, axis=0, keepdims=True)
        out_ref[1:2, :] = jnp.sum(squares, axis=0, keepdims=True)

    return pl.pallas_call(
        body,
        name="spatial_stage",
        in_specs=[SM] + [HBM] * 3 + [VM] * 3,
        out_specs=[VM] * 5,
        out_shape=[
            jax.ShapeDtypeStruct((rows, middle), jnp.float32),
            jax.ShapeDtypeStruct((2, middle), jnp.float32),
            jax.ShapeDtypeStruct((1, middle), jnp.float32),
            jax.ShapeDtypeStruct((1, middle), jnp.float32),
            jax.ShapeDtypeStruct((shards_of * each, 2 * pieces * lane), jnp.bfloat16),
        ],
        scratch_shapes=[
            pltpu.VMEM((side + 2, wide, middle), jnp.bfloat16),
            pltpu.VMEM((mixed, middle), jnp.bfloat16),
            pltpu.VMEM((rows, middle), jnp.float32),
            pltpu.VMEM((2, shards_of, packed, lane), jnp.bfloat16),
            pltpu.SemaphoreType.DMA((side,)),
            pltpu.SemaphoreType.DMA((2,)),
        ],
        compiler_params=pltpu.CompilerParams(vmem_limit_bytes=24 << 20),
        cost_estimate=cost(2 * rows * mixed * middle),
    )(own, *in_hbm(reduced, mine, other), sums, gain, bias)


def second_stage(spatial, sums, gain, bias, weight, side, images, row_count):
    rows, middle = spatial.shape
    channels = weight.shape[1]
    chunk = side * images

    def body(spatial_ref, sums_ref, gain_ref, bias_ref, weight_ref, second_ref, out_ref,
             mean_ref, var_ref):
        mean, var = moments(sums_ref[...], row_count)
        mean_ref[...] = mean
        var_ref[...] = var
        scale = lax.rsqrt(var + EPSILON) * gain_ref[...]
        shift = bias_ref[...] - mean * scale

        def one(step, carry):
            total, gram = carry
            part = pl.ds(step * chunk, chunk)
            values = jnp.maximum(spatial_ref[part, :] * scale + shift, 0.0).astype(jnp.bfloat16)
            second_ref[part, :] = values
            gram = gram + lax.dot_general(
                values, values, (((0,), (0,)), ((), ())), preferred_element_type=jnp.float32
            )
            return total + column_sums(values.astype(jnp.float32)), gram

        total, gram = lax.fori_loop(
            0,
            side,
            one,
            (jnp.zeros((8, middle), jnp.float32), jnp.zeros((middle, middle), jnp.float32)),
        )
        stacked = jnp.concatenate([gram, total], axis=0)
        high = stacked.astype(jnp.bfloat16)
        rest = stacked - high.astype(jnp.float32)
        mid = rest.astype(jnp.bfloat16)
        low = (rest - mid.astype(jnp.float32)).astype(jnp.bfloat16)
        kernel = weight_ref[...]
        product = (
            jnp.dot(low, kernel, preferred_element_type=jnp.float32)
            + jnp.dot(mid, kernel, preferred_element_type=jnp.float32)
            + jnp.dot(high, kernel, preferred_element_type=jnp.float32)
        )
        out_ref[0:1, :] = jnp.sum(product[middle:], axis=0, keepdims=True)
        out_ref[1:2, :] = jnp.sum(
            product[:middle] * kernel.astype(jnp.float32), axis=0, keepdims=True
        )

    return pl.pallas_call(
        body,
        name="second_stage",
        in_specs=[VM] * 5,
        out_specs=[VM] * 4,
        out_shape=[
            jax.ShapeDtypeStruct((rows, middle), jnp.bfloat16),
            jax.ShapeDtypeStruct((2, channels), jnp.float32),
            jax.ShapeDtypeStruct((1, middle), jnp.float32),
            jax.ShapeDtypeStruct((1, middle), jnp.float32),
        ],
        compiler_params=pltpu.CompilerParams(vmem_limit_bytes=16 << 20),
        cost_estimate=cost(2 * rows * middle * middle),
    )(spatial, sums, gain, bias, weight)


def output_stage(second, maps, sums, gain, bias, weight, side, images, row_count):
    rows, middle = second.shape
    channels = weight.shape[1]
    chunk = side * images
    tiles = 4
    width = channels // tiles

    def body(second_ref, maps_ref, sums_ref, gain_ref, bias_ref, weight_ref, out_ref, mean_ref,
             var_ref, pooled_ref, held_ref, sems):
        def copy(step):
            part = pl.ds(step * chunk, chunk)
            return pltpu.make_async_copy(maps_ref.at[part], held_ref.at[part], sems.at[step])

        for step in range(side):
            copy(step).start()
        mean, var = moments(sums_ref[...], row_count)
        mean_ref[...] = mean
        var_ref[...] = var
        scale_all = lax.rsqrt(var + EPSILON) * gain_ref[...]
        shift_all = bias_ref[...] - mean * scale_all
        pooled_ref[...] = jnp.zeros((images, channels), jnp.float32)

        def one(step, carry):
            copy(step).wait()
            part = pl.ds(step * chunk, chunk)
            for tile in range(tiles):
                cols = slice(tile * width, (tile + 1) * width)
                product = jnp.dot(
                    second_ref[part, :], weight_ref[:, cols], preferred_element_type=jnp.float32
                )
                values = product * scale_all[:, cols] + (
                    shift_all[:, cols] + held_ref[part, cols].astype(jnp.float32)
                )
                values = jnp.maximum(values, 0.0)
                pooled_ref[:, cols] += jnp.sum(values.reshape(side, images, width), axis=0)
            return carry

        lax.fori_loop(0, side, one, 0)
        out_ref[...] = (pooled_ref[...] * (1.0 / (side * side))).astype(jnp.bfloat16)

    return pl.pallas_call(
        body,
        name="output_stage",
        in_specs=[VM, HBM] + [VM] * 4,
        out_specs=[VM] * 3,
        out_shape=[
            jax.ShapeDtypeStruct((images, channels), jnp.bfloat16),
            jax.ShapeDtypeStruct((1, channels), jnp.float32),
            jax.ShapeDtypeStruct((1, channels), jnp.float32),
        ],
        scratch_shapes=[
            pltpu.VMEM((images, channels), jnp.float32),
            pltpu.VMEM((rows, channels), jnp.bfloat16),
            pltpu.SemaphoreType.DMA((side,)),
        ],
        compiler_params=pltpu.CompilerParams(vmem_limit_bytes=24 << 20),
        cost_estimate=cost(2 * rows * channels * middle),
    )(second, maps, sums, gain, bias, weight)


def probe_stage(own, pooled, mine, other, first_row, shift, labels, image_count):
    images, channels = pooled.shape
    lanes = shift.shape[1]
    shards_of, packed, lane = mine.shape
    class_rows = packed - first_row
    cols = channels // shards_of
    tiles = class_rows // cols

    def body(own_ref, labels_ref, pooled_ref, mine_ref, other_ref, shift_ref, margin_ref,
             halves_ref, sems):
        core = own_ref[1]
        rows_of = pl.ds(first_row, class_rows)
        fetch(
            [
                (mine_ref.at[:, rows_of, :], halves_ref.at[core]),
                (other_ref.at[:, rows_of, :], halves_ref.at[1 - core]),
            ],
            sems,
        )
        parts = []
        for half in range(2):
            for pair in range(tiles // 2):
                kernel = jnp.concatenate(
                    [
                        halves_ref[half, :, tile * cols : (tile + 1) * cols, :].reshape(
                            channels, lane
                        )
                        for tile in (2 * pair, 2 * pair + 1)
                    ],
                    axis=1,
                )
                parts.append(
                    jnp.dot(pooled_ref[...], kernel, preferred_element_type=jnp.float32)
                )
        logits = jnp.concatenate(parts, axis=1) + shift_ref[...]
        index = lax.broadcasted_iota(jnp.int32, (images, 1), 0)
        column = jnp.zeros((images, 1), jnp.int32)
        for image in range(images):
            column = jnp.where(index == image, labels_ref[image], column)
        onehot = lax.broadcasted_iota(jnp.int32, (images, lanes), 1) == column
        correct = jnp.sum(jnp.where(onehot, logits, 0.0), axis=1, keepdims=True)
        rivals = jnp.max(jnp.where(onehot, -1e30, logits), axis=1, keepdims=True)
        total = jnp.sum(correct - rivals, axis=0, keepdims=True) * (1.0 / image_count)
        margin_ref[...] = jnp.broadcast_to(total, (1, 128))

    return pl.pallas_call(
        body,
        name="probe_stage",
        in_specs=[SM, SM, VM, HBM, HBM, VM],
        out_specs=VM,
        out_shape=jax.ShapeDtypeStruct((1, 128), jnp.float32),
        scratch_shapes=[
            pltpu.VMEM((2, shards_of, class_rows, lane), jnp.bfloat16),
            pltpu.SemaphoreType.DMA((2,)),
        ],
        compiler_params=pltpu.CompilerParams(vmem_limit_bytes=12 << 20),
    )(own, labels, pooled, *in_hbm(mine, other), shift)


def shards(activations, labels, t_values, point_index, w_reduce, w_spatial, w_expand, w_classes,
           norm_gain, norm_bias, class_bias):
    images, side, _, channels = activations.shape
    middle = w_reduce.shape[2]
    image_count = images * lax.axis_size(BATCH)
    row_count = float(image_count * side * side)
    lanes = -(-class_bias.shape[1] // 128) * 128
    own = jnp.stack([lax.axis_index(POINT), lax.axis_index("core")]).astype(jnp.int32)
    sent, gain, bias, shift = first_weights(
        t_values, point_index, own, w_reduce, norm_gain, norm_bias, class_bias, lanes
    )
    reduce_w = exchange(sent).reshape(channels, middle)
    packed = other_weights(
        t_values, point_index, own, w_spatial, w_expand, jnp.swapaxes(w_classes, 1, 2), lanes
    )
    packed, reduce_w = lax.optimization_barrier((packed, reduce_w))
    mine = exchange(packed)
    maps = jnp.transpose(activations, (1, 2, 0, 3)).reshape(side * side * images, channels)
    maps = pltpu.with_memory_space_constraint(maps, pltpu.HBM)
    reduced, sums = reduce_stage(maps, reduce_w, side, images)
    sums = batch_sum(sums)
    mine, sums = lax.optimization_barrier((mine, sums))
    other = lax.ppermute(mine, "core", [(0, 1), (1, 0)])
    taps = w_spatial.shape[1]
    expand_rows = w_expand.shape[1]
    spatial, sums, mean_one, var_one, expand_w = spatial_stage(
        own, reduced, sums, gain[:, :middle], bias[:, :middle], mine, other, taps, expand_rows,
        side, images, row_count
    )
    sums = batch_sum(sums)
    second, sums, mean_two, var_two = second_stage(
        spatial, sums, gain[:, middle : 2 * middle], bias[:, middle : 2 * middle], expand_w,
        side, images, row_count
    )
    sums = batch_sum(sums)
    pooled, mean_three, var_three = output_stage(
        second, maps, sums, gain[:, 2 * middle :], bias[:, 2 * middle :], expand_w, side, images,
        row_count
    )
    margin = probe_stage(
        own, pooled, mine, other, taps + 4 * expand_rows, shift, labels, image_count
    )
    margin = batch_sum(margin)
    points = lax.axis_size(POINT)
    copies = jnp.broadcast_to(margin[None], (points, 1, 128))
    margin_all = exchange(copies)[:, 0, 0]
    return mean_one, var_one, mean_two, var_two, mean_three, var_three, margin_all


def solution(mesh):
    torus = Mesh(mesh.devices.reshape(2, 4, 4, 2, 2), POINT + BATCH)
    rows = P(POINT, None)
    return jax.shard_map(
        shards,
        mesh=torus,
        in_specs=(
            P(BATCH, None, None, None),
            P(BATCH),
            P(),
            P(),
            P(None, POINT, None),
            P(None, POINT, None),
            P(None, POINT, None),
            P(None, None, POINT),
            P(),
            P(),
            P(),
        ),
        out_specs=(rows, rows, rows, rows, rows, rows, P()),
        check_vma=False,
    )
```

```python
import jax
import jax.numpy as jnp
from jax import lax
from jax.experimental import pallas as pl
from jax.experimental.pallas import tpu as pltpu
from jax.sharding import Mesh
from jax.sharding import PartitionSpec as P

POINT = ("pz", "px", "py")
BATCH = ("bz", "core")
EPSILON = 1e-05
PAIR = 2
SM = pl.BlockSpec(memory_space=pltpu.SMEM)
VM = pl.BlockSpec(memory_space=pltpu.VMEM)
HBM = pl.BlockSpec(memory_space=pltpu.HBM)


def coefficients_of(values_ref, index_ref, point):
    doubled = 2.0 * values_ref[index_ref[point]]
    return (
        jnp.maximum(1.0 - doubled, 0.0),
        1.0 - jnp.abs(1.0 - doubled),
        jnp.maximum(doubled - 1.0, 0.0),
    )


def blend(row, parts):
    return row[0] * parts[0] + row[1] * parts[1] + row[2] * parts[2]


def fetch(pairs, sems):
    copies = [
        pltpu.make_async_copy(source, target, sems.at[k])
        for k, (source, target) in enumerate(pairs)
    ]
    for copy in copies:
        copy.start()
    for copy in copies:
        copy.wait()


def in_hbm(*arrays):
    return [pltpu.with_memory_space_constraint(x, pltpu.HBM) for x in arrays]


def first_weights(t_values, point_index, own, w_reduce, gains, biases, class_bias, lanes):
    _, rows, middle = w_reduce.shape
    points = point_index.shape[0]
    classes = class_bias.shape[1]

    def body(own_ref, *refs):
        sources = refs[:6]
        out_ref, gain_ref, bias_ref, shift_ref = refs[6:10]
        values_ref, index_ref, reduce_ref, gains_ref, biases_ref, class_ref = refs[10:16]
        wide_ref, sems = refs[16:]
        fetch(list(zip(sources, refs[10:16])), sems)
        wide_ref[...] = reduce_ref[...].astype(jnp.float32)

        def one(point, carry):
            row = coefficients_of(values_ref, index_ref, point)
            out_ref[point] = blend(row, wide_ref).astype(jnp.bfloat16)
            return carry

        lax.fori_loop(0, points, one, 0)
        row = coefficients_of(values_ref, index_ref, own_ref[0])

        def ends(ref):
            return [ref[k : k + 1, :] for k in range(3)]

        gain_ref[...] = blend(row, ends(gains_ref))
        bias_ref[...] = blend(row, ends(biases_ref))
        shift_ref[...] = jnp.full((1, lanes), -1e30, jnp.float32)
        shift_ref[:, :classes] = blend(row, ends(class_ref))

    return pl.pallas_call(
        body,
        name="first_weights",
        in_specs=[SM] + [HBM] * 6,
        out_specs=[VM] * 4,
        out_shape=[
            jax.ShapeDtypeStruct((points, rows, middle), jnp.bfloat16),
            jax.ShapeDtypeStruct((1, gains.shape[1]), jnp.float32),
            jax.ShapeDtypeStruct((1, biases.shape[1]), jnp.float32),
            jax.ShapeDtypeStruct((1, lanes), jnp.float32),
        ],
        scratch_shapes=[
            pltpu.SMEM(t_values.shape, jnp.float32),
            pltpu.SMEM(point_index.shape, jnp.int32),
            pltpu.VMEM(w_reduce.shape, w_reduce.dtype),
            pltpu.VMEM(gains.shape, jnp.float32),
            pltpu.VMEM(biases.shape, jnp.float32),
            pltpu.VMEM(class_bias.shape, jnp.float32),
            pltpu.VMEM(w_reduce.shape, jnp.float32),
            pltpu.SemaphoreType.DMA((6,)),
        ],
        compiler_params=pltpu.CompilerParams(vmem_limit_bytes=16 << 20),
    )(own, *in_hbm(t_values, point_index, w_reduce, gains, biases, class_bias))


def other_weights(t_values, point_index, own, w_spatial, w_expand, w_classes, lanes):
    _, taps, middle = w_spatial.shape
    _, rows, channels = w_expand.shape
    _, cols, classes = w_classes.shape
    points = point_index.shape[0]
    lane = middle // 2
    tiles = channels // (2 * lane)
    class_tiles = lanes // (2 * lane)
    conv_rows = taps + tiles * rows
    packed = conv_rows + class_tiles * cols
    groups = 4
    each = points // groups

    def body(own_ref, values_in, index_in, spatial_in, expand_in, classes_in, out_ref,
             values_ref, index_ref, spatial_ref, expand_ref, classes_ref, packed_ref, wide_ref,
             block_ref, sems, out_sems):
        fetch(
            [
                (values_in, values_ref),
                (index_in, index_ref),
                (spatial_in, spatial_ref),
                (expand_in, expand_ref),
                (classes_in, classes_ref),
            ],
            sems,
        )
        low = own_ref[1] == 0
        wide_ref[...] = jnp.zeros(wide_ref.shape, jnp.float32)
        wide_ref[:, :, :classes] = classes_ref[...].astype(jnp.float32)

        def half(ref, tile, tiles_of):
            first = ref[:, :, tile * lane : (tile + 1) * lane].astype(jnp.float32)
            start = (tiles_of + tile) * lane
            last = ref[:, :, start : start + lane].astype(jnp.float32)
            return jnp.where(low, first, last)

        packed_ref[:, :taps, :] = half(spatial_ref, 0, 1)
        for tile in range(tiles):
            start = taps + tile * rows
            packed_ref[:, start : start + rows, :] = half(expand_ref, tile, tiles)
        for tile in range(class_tiles):
            start = conv_rows + tile * cols
            packed_ref[:, start : start + cols, :] = half(wide_ref, tile, class_tiles)

        def copy_out(group):
            part = pl.ds(group * each, each)
            return pltpu.make_async_copy(
                block_ref.at[part], out_ref.at[part], out_sems.at[group]
            )

        def one(point, carry):
            row = coefficients_of(values_ref, index_ref, point)
            block_ref[point] = blend(row, packed_ref).astype(jnp.bfloat16)
            return carry

        for group in range(groups):
            lax.fori_loop(group * each, (group + 1) * each, one, 0)
            copy_out(group).start()
        for group in range(groups):
            copy_out(group).wait()

    return pl.pallas_call(
        body,
        name="other_weights",
        in_specs=[SM] + [HBM] * 5,
        out_specs=HBM,
        out_shape=pltpu.HBM((points, packed, lane), jnp.bfloat16),
        scratch_shapes=[
            pltpu.SMEM(t_values.shape, jnp.float32),
            pltpu.SMEM(point_index.shape, jnp.int32),
            pltpu.VMEM(w_spatial.shape, w_spatial.dtype),
            pltpu.VMEM(w_expand.shape, w_expand.dtype),
            pltpu.VMEM(w_classes.shape, w_classes.dtype),
            pltpu.VMEM((3, packed, lane), jnp.float32),
            pltpu.VMEM((3, cols, lanes), jnp.float32),
            pltpu.VMEM((points, packed, lane), jnp.bfloat16),
            pltpu.SemaphoreType.DMA((5,)),
            pltpu.SemaphoreType.DMA((groups,)),
        ],
        compiler_params=pltpu.CompilerParams(vmem_limit_bytes=16 << 20),
    )(own, *in_hbm(t_values, point_index, w_spatial, w_expand, w_classes))


def exchange(x):
    return lax.all_to_all(x, POINT, split_axis=0, concat_axis=0, tiled=True)


def batch_sum(x):
    x = x + lax.ppermute(x, "core", [(0, 1), (1, 0)])
    return x + lax.ppermute(x, "bz", [(0, 1), (1, 0)])


def cost(flops):
    return pl.CostEstimate(flops=flops, transcendentals=0, bytes_accessed=flops // 512)


def column_sums(x):
    return jnp.sum(x.reshape(x.shape[0] // 8, 8, x.shape[1]), axis=0)


def moments(sums, rows):
    mean = sums[0:1] * (1.0 / rows)
    var = sums[1:2] * (1.0 / rows) - mean * mean
    return mean, var


def reduce_stage(maps, weight, side, images):
    rows, channels = maps.shape
    middle = weight.shape[1]
    chunk = PAIR * side * images
    steps = side // PAIR

    def body(maps_ref, weight_ref, reduced_ref, sums_ref, held_ref, block_ref, sems, out_sems):
        def copy(step):
            part = pl.ds(step * chunk, chunk)
            return pltpu.make_async_copy(maps_ref.at[part], held_ref.at[part], sems.at[step])

        def copy_out(step):
            part = pl.ds(step * chunk, chunk)
            return pltpu.make_async_copy(
                block_ref.at[part], reduced_ref.at[part], out_sems.at[step]
            )

        for step in range(steps):
            copy(step).start()

        def one(step, carry):
            total, squares = carry
            copy(step).wait()
            part = pl.ds(step * chunk, chunk)
            product = jnp.dot(
                held_ref[part, :], weight_ref[...], preferred_element_type=jnp.float32
            )
            block_ref[part, :] = product
            copy_out(step).start()
            return total + column_sums(product), squares + column_sums(product * product)

        zero = jnp.zeros((8, middle), jnp.float32)
        total, squares = lax.fori_loop(0, steps, one, (zero, zero))
        sums_ref[0:1, :] = jnp.sum(total, axis=0, keepdims=True)
        sums_ref[1:2, :] = jnp.sum(squares, axis=0, keepdims=True)
        for step in range(steps):
            copy_out(step).wait()

    return pl.pallas_call(
        body,
        name="reduce_stage",
        in_specs=[HBM, VM],
        out_specs=[HBM, VM],
        out_shape=[
            pltpu.HBM((rows, middle), jnp.float32),
            jax.ShapeDtypeStruct((2, middle), jnp.float32),
        ],
        scratch_shapes=[
            pltpu.VMEM((rows, channels), jnp.bfloat16),
            pltpu.VMEM((rows, middle), jnp.float32),
            pltpu.SemaphoreType.DMA((steps,)),
            pltpu.SemaphoreType.DMA((steps,)),
        ],
        compiler_params=pltpu.CompilerParams(vmem_limit_bytes=32 << 20),
        cost_estimate=cost(2 * rows * channels * middle),
    )(maps, weight)


def spatial_stage(own, reduced, sums, gain, bias, mine, other, taps, expand_rows, side, images,
                  row_count):
    rows, middle = reduced.shape
    shards_of, _, lane = mine.shape
    mixed = shards_of * taps
    pieces = 4
    each = expand_rows
    packed = taps + pieces * each
    chunk = side * images
    wide = chunk + 2 * images

    def body(own_ref, reduced_ref, mine_ref, other_ref, sums_ref, gain_ref, bias_ref,
             spatial_ref, out_ref, mean_ref, var_ref, expand_ref, first_ref, weight_ref, held_ref,
             halves_ref, sems):
        core = own_ref[1]
        low = core == 0

        def copy(step):
            part = pl.ds(step * chunk, chunk)
            return pltpu.make_async_copy(reduced_ref.at[part], held_ref.at[part], sems.at[step])

        for step in range(side):
            copy(step).start()
        mean, var = moments(sums_ref[...], row_count)
        mean_ref[...] = mean
        var_ref[...] = var
        scale = lax.rsqrt(var + EPSILON) * gain_ref[...]
        shift = bias_ref[...] - mean * scale
        edge = jnp.zeros((images, middle), jnp.bfloat16)
        first_ref[0] = jnp.zeros((wide, middle), jnp.bfloat16)
        first_ref[side + 1] = jnp.zeros((wide, middle), jnp.bfloat16)

        def norm(row, carry):
            copy(row).wait()
            values = held_ref[pl.ds(row * chunk, chunk), :]
            values = jnp.maximum(values * scale + shift, 0.0)
            first_ref[row + 1, 0:images, :] = edge
            first_ref[row + 1, images : images + chunk, :] = values.astype(jnp.bfloat16)
            first_ref[row + 1, images + chunk :, :] = edge
            return carry

        lax.fori_loop(0, side, norm, 0)
        for half in range(2):
            first = jnp.where(low, mine_ref[...], other_ref[...])
            last = jnp.where(low, other_ref[...], mine_ref[...])
            halves_ref[...] = (first, last)[half]
            weight_ref[:, half * lane : (half + 1) * lane] = (
                halves_ref[:, :taps, :]
                .astype(jnp.float32)
                .reshape(mixed, lane)
                .astype(jnp.bfloat16)
            )
            for piece in range(pieces):
                start = taps + piece * each
                column = (half * pieces + piece) * lane
                expand_ref[:, column : column + lane] = (
                    halves_ref[:, start : start + each, :]
                    .astype(jnp.float32)
                    .reshape(shards_of * each, lane)
                    .astype(jnp.bfloat16)
                )

        def one(step, carry):
            total, squares = carry
            windows = [
                first_ref[
                    pl.ds(PAIR * step + dy, PAIR), dx * images : dx * images + chunk, :
                ].reshape(PAIR * chunk, middle)
                for dy in range(3)
                for dx in range(3)
            ]
            product = sum(
                jnp.dot(
                    window,
                    weight_ref[tap * middle : (tap + 1) * middle, :],
                    preferred_element_type=jnp.float32,
                )
                for tap, window in enumerate(windows)
            )
            spatial_ref[pl.ds(step * PAIR * chunk, PAIR * chunk), :] = product
            return total + column_sums(product), squares + column_sums(product * product)

        zero = jnp.zeros((8, middle), jnp.float32)
        total, squares = lax.fori_loop(0, side // PAIR, one, (zero, zero))
        out_ref[0:1, :] = jnp.sum(total, axis=0, keepdims=True)
        out_ref[1:2, :] = jnp.sum(squares, axis=0, keepdims=True)

    return pl.pallas_call(
        body,
        name="spatial_stage",
        in_specs=[SM, HBM] + [VM] * 5,
        out_specs=[VM] * 5,
        out_shape=[
            jax.ShapeDtypeStruct((rows, middle), jnp.float32),
            jax.ShapeDtypeStruct((2, middle), jnp.float32),
            jax.ShapeDtypeStruct((1, middle), jnp.float32),
            jax.ShapeDtypeStruct((1, middle), jnp.float32),
            jax.ShapeDtypeStruct((shards_of * each, 2 * pieces * lane), jnp.bfloat16),
        ],
        scratch_shapes=[
            pltpu.VMEM((side + 2, wide, middle), jnp.bfloat16),
            pltpu.VMEM((mixed, middle), jnp.bfloat16),
            pltpu.VMEM((rows, middle), jnp.float32),
            pltpu.VMEM((shards_of, packed, lane), jnp.bfloat16),
            pltpu.SemaphoreType.DMA((side,)),
        ],
        compiler_params=pltpu.CompilerParams(vmem_limit_bytes=24 << 20),
        cost_estimate=cost(2 * rows * mixed * middle),
    )(own, *in_hbm(reduced), mine, other, sums, gain, bias)


def second_stage(spatial, sums, gain, bias, weight, side, images, row_count):
    rows, middle = spatial.shape
    channels = weight.shape[1]
    chunk = PAIR * side * images

    def body(spatial_ref, sums_ref, gain_ref, bias_ref, weight_ref, second_ref, out_ref,
             mean_ref, var_ref):
        mean, var = moments(sums_ref[...], row_count)
        mean_ref[...] = mean
        var_ref[...] = var
        scale = lax.rsqrt(var + EPSILON) * gain_ref[...]
        shift = bias_ref[...] - mean * scale

        def one(step, carry):
            total, gram = carry
            part = pl.ds(step * chunk, chunk)
            values = jnp.maximum(spatial_ref[part, :] * scale + shift, 0.0).astype(jnp.bfloat16)
            second_ref[part, :] = values
            gram = gram + lax.dot_general(
                values, values, (((0,), (0,)), ((), ())), preferred_element_type=jnp.float32
            )
            return total + column_sums(values.astype(jnp.float32)), gram

        total, gram = lax.fori_loop(
            0,
            side // PAIR,
            one,
            (jnp.zeros((8, middle), jnp.float32), jnp.zeros((middle, middle), jnp.float32)),
        )
        stacked = jnp.concatenate([gram, total], axis=0)
        high = stacked.astype(jnp.bfloat16)
        rest = stacked - high.astype(jnp.float32)
        mid = rest.astype(jnp.bfloat16)
        low = (rest - mid.astype(jnp.float32)).astype(jnp.bfloat16)
        kernel = weight_ref[...]
        product = (
            jnp.dot(low, kernel, preferred_element_type=jnp.float32)
            + jnp.dot(mid, kernel, preferred_element_type=jnp.float32)
            + jnp.dot(high, kernel, preferred_element_type=jnp.float32)
        )
        out_ref[0:1, :] = jnp.sum(product[middle:], axis=0, keepdims=True)
        out_ref[1:2, :] = jnp.sum(
            product[:middle] * kernel.astype(jnp.float32), axis=0, keepdims=True
        )

    return pl.pallas_call(
        body,
        name="second_stage",
        in_specs=[VM] * 5,
        out_specs=[VM] * 4,
        out_shape=[
            jax.ShapeDtypeStruct((rows, middle), jnp.bfloat16),
            jax.ShapeDtypeStruct((2, channels), jnp.float32),
            jax.ShapeDtypeStruct((1, middle), jnp.float32),
            jax.ShapeDtypeStruct((1, middle), jnp.float32),
        ],
        compiler_params=pltpu.CompilerParams(vmem_limit_bytes=16 << 20),
        cost_estimate=cost(2 * rows * middle * middle),
    )(spatial, sums, gain, bias, weight)


def output_stage(second, maps, sums, gain, bias, weight, side, images, row_count):
    rows, middle = second.shape
    channels = weight.shape[1]
    chunk = side * images
    tiles = 4
    width = channels // tiles

    def body(second_ref, maps_ref, sums_ref, gain_ref, bias_ref, weight_ref, out_ref, mean_ref,
             var_ref, pooled_ref, held_ref, sems):
        def copy(step):
            part = pl.ds(step * chunk, chunk)
            return pltpu.make_async_copy(maps_ref.at[part], held_ref.at[part], sems.at[step])

        for step in range(side):
            copy(step).start()
        mean, var = moments(sums_ref[...], row_count)
        mean_ref[...] = mean
        var_ref[...] = var
        scale_all = lax.rsqrt(var + EPSILON) * gain_ref[...]
        shift_all = bias_ref[...] - mean * scale_all
        pooled_ref[...] = jnp.zeros((images, channels), jnp.float32)

        def one(step, carry):
            copy(step).wait()
            part = pl.ds(step * chunk, chunk)
            for tile in range(tiles):
                cols = slice(tile * width, (tile + 1) * width)
                product = jnp.dot(
                    second_ref[part, :], weight_ref[:, cols], preferred_element_type=jnp.float32
                )
                values = product * scale_all[:, cols] + (
                    shift_all[:, cols] + held_ref[part, cols].astype(jnp.float32)
                )
                values = jnp.maximum(values, 0.0)
                pooled_ref[:, cols] += jnp.sum(values.reshape(side, images, width), axis=0)
            return carry

        lax.fori_loop(0, side, one, 0)
        out_ref[...] = (pooled_ref[...] * (1.0 / (side * side))).astype(jnp.bfloat16)

    return pl.pallas_call(
        body,
        name="output_stage",
        in_specs=[VM, HBM] + [VM] * 4,
        out_specs=[VM] * 3,
        out_shape=[
            jax.ShapeDtypeStruct((images, channels), jnp.bfloat16),
            jax.ShapeDtypeStruct((1, channels), jnp.float32),
            jax.ShapeDtypeStruct((1, channels), jnp.float32),
        ],
        scratch_shapes=[
            pltpu.VMEM((images, channels), jnp.float32),
            pltpu.VMEM((rows, channels), jnp.bfloat16),
            pltpu.SemaphoreType.DMA((side,)),
        ],
        compiler_params=pltpu.CompilerParams(vmem_limit_bytes=24 << 20),
        cost_estimate=cost(2 * rows * channels * middle),
    )(second, maps, sums, gain, bias, weight)


def probe_stage(own, pooled, mine, other, shift, labels, image_count):
    images, channels = pooled.shape
    lanes = shift.shape[1]
    shards_of, class_rows, lane = mine.shape
    cols = channels // shards_of
    tiles = class_rows // cols

    def body(own_ref, labels_ref, pooled_ref, mine_ref, other_ref, shift_ref, margin_ref):
        low = own_ref[1] == 0
        parts = []
        for half in range(2):
            for pair in range(tiles // 2):
                kernel = jnp.concatenate(
                    [
                        jnp.where(
                            low,
                            (mine_ref, other_ref)[half][:, tile * cols : (tile + 1) * cols, :],
                            (other_ref, mine_ref)[half][:, tile * cols : (tile + 1) * cols, :],
                        ).reshape(channels, lane)
                        for tile in (2 * pair, 2 * pair + 1)
                    ],
                    axis=1,
                )
                parts.append(
                    jnp.dot(pooled_ref[...], kernel, preferred_element_type=jnp.float32)
                )
        logits = jnp.concatenate(parts, axis=1) + shift_ref[...]
        index = lax.broadcasted_iota(jnp.int32, (images, 1), 0)
        column = jnp.zeros((images, 1), jnp.int32)
        for image in range(images):
            column = jnp.where(index == image, labels_ref[image], column)
        onehot = lax.broadcasted_iota(jnp.int32, (images, lanes), 1) == column
        correct = jnp.sum(jnp.where(onehot, logits, 0.0), axis=1, keepdims=True)
        rivals = jnp.max(jnp.where(onehot, -1e30, logits), axis=1, keepdims=True)
        total = jnp.sum(correct - rivals, axis=0, keepdims=True) * (1.0 / image_count)
        margin_ref[...] = jnp.broadcast_to(total, (1, 128))

    return pl.pallas_call(
        body,
        name="probe_stage",
        in_specs=[SM, SM, VM, VM, VM, VM],
        out_specs=VM,
        out_shape=jax.ShapeDtypeStruct((1, 128), jnp.float32),
        compiler_params=pltpu.CompilerParams(vmem_limit_bytes=12 << 20),
    )(own, labels, pooled, mine, other, shift)


def shards(activations, labels, t_values, point_index, w_reduce, w_spatial, w_expand, w_classes,
           norm_gain, norm_bias, class_bias):
    images, side, _, channels = activations.shape
    middle = w_reduce.shape[2]
    image_count = images * lax.axis_size(BATCH)
    row_count = float(image_count * side * side)
    lanes = -(-class_bias.shape[1] // 128) * 128
    own = jnp.stack([lax.axis_index(POINT), lax.axis_index("core")]).astype(jnp.int32)
    sent, gain, bias, shift = first_weights(
        t_values, point_index, own, w_reduce, norm_gain, norm_bias, class_bias, lanes
    )
    reduce_w = exchange(sent).reshape(channels, middle)
    packed = other_weights(
        t_values, point_index, own, w_spatial, w_expand, jnp.swapaxes(w_classes, 1, 2), lanes
    )
    packed, reduce_w = lax.optimization_barrier((packed, reduce_w))
    mine = exchange(packed)
    maps = jnp.transpose(activations, (1, 2, 0, 3)).reshape(side * side * images, channels)
    maps = pltpu.with_memory_space_constraint(maps, pltpu.HBM)
    reduced, sums = reduce_stage(maps, reduce_w, side, images)
    sums = batch_sum(sums)
    mine, sums = lax.optimization_barrier((mine, sums))
    taps = w_spatial.shape[1]
    expand_rows = w_expand.shape[1]
    conv_rows = taps + channels // middle * expand_rows
    swap = [(0, 1), (1, 0)]
    mine, class_mine = mine[:, :conv_rows], mine[:, conv_rows:]
    other = lax.ppermute(mine, "core", swap)
    class_mine, other = lax.optimization_barrier((class_mine, other))
    class_other = lax.ppermute(class_mine, "core", swap)
    spatial, sums, mean_one, var_one, expand_w = spatial_stage(
        own, reduced, sums, gain[:, :middle], bias[:, :middle], mine, other, taps, expand_rows,
        side, images, row_count
    )
    sums = batch_sum(sums)
    second, sums, mean_two, var_two = second_stage(
        spatial, sums, gain[:, middle : 2 * middle], bias[:, middle : 2 * middle], expand_w,
        side, images, row_count
    )
    sums = batch_sum(sums)
    pooled, mean_three, var_three = output_stage(
        second, maps, sums, gain[:, 2 * middle :], bias[:, 2 * middle :], expand_w, side, images,
        row_count
    )
    margin = probe_stage(
        own, pooled, class_mine, class_other, shift, labels, image_count
    )
    margin = batch_sum(margin)
    points = lax.axis_size(POINT)
    copies = jnp.broadcast_to(margin[None], (points, 1, 128))
    margin_all = exchange(copies)[:, 0, 0]
    return mean_one, var_one, mean_two, var_two, mean_three, var_three, margin_all


def solution(mesh):
    torus = Mesh(mesh.devices.reshape(2, 4, 4, 2, 2), POINT + BATCH)
    rows = P(POINT, None)
    return jax.shard_map(
        shards,
        mesh=torus,
        in_specs=(
            P(BATCH, None, None, None),
            P(BATCH),
            P(),
            P(),
            P(None, POINT, None),
            P(None, POINT, None),
            P(None, POINT, None),
            P(None, None, POINT),
            P(),
            P(),
            P(),
        ),
        out_specs=(rows, rows, rows, rows, rows, rows, P()),
        check_vma=False,
    )
```
